32 devices in a mesh: dp: 16 (over z, x, core), mp: 2 (over y).
Axes of the slice: x: 2, y: 2, z: 4, core: 2. Of those that a mesh axis runs over, the one named last changes fastest.
Arguments:
- ranges: bfloat16 [512, 2652], P(('dp', 'mp')), may hold values from 0.0099487305 to 1
- board: int32 [512, 5], P(('dp', 'mp')), may hold values from 0 to 51, as said below
- targets: bfloat16 [512, 2652], P(('dp', 'mp')), may hold values from -6 to 6
- w_in: bfloat16 [1536, 2704], P(('mp', 'dp')), may hold values from -0.34570312 to 0.34570312
- w_out: bfloat16 [1536, 2652], P(('mp', 'dp')), may hold values from -0.3046875 to 0.3046875
Outputs:
- predicted: bfloat16 [512, 2652], P(('dp', 'mp'))
- update_in: float32 [1536, 2704], P(('mp', 'dp'))
- update_out: float32 [1536, 2652], P(('mp', 'dp'))
- loss: float32 [], replicated
The draws below stay inside these ranges and needn't reach their ends.
Inputs may be any that keep to these rules, and one draw needn't show every extreme that they name: `board`: each row holds 5 different cards.
All inputs are finite; a program needn't handle non-finite values.
Results may differ from the reference program's by a relative error of at most 0.014.
Values may be sent and summed in bfloat16 or wider, within the bound.
A program may use at most 64 MiB of HBM per device.

```python
import math
import jax
import jax.numpy as jnp
from jax import lax

CARDS = 52
BOARD = 5
HIDDEN_SIZE = 1536
INW = 2704
OUTW = 2652
BATCH = 512
N_MP = 2


def draw_board(key, part):
    row_keys = jax.random.split(key, BATCH)

    def one_board(row_key):
        return jax.random.permutation(row_key, CARDS)[:BOARD]
    return jax.vmap(one_board)(row_keys).astype(jnp.int32)


def block_levels(key, shape, pieces, low, high):
    factor_of = 1.0
    for dim, blocks in pieces:
        draws = jax.random.uniform(jax.random.fold_in(jax.random.fold_in(key, 6), dim), (blocks,), jnp.float32, low / len(pieces), high / len(pieces))
        factor_of = factor_of * jnp.repeat(jnp.exp(draws), shape[dim] // blocks).reshape((-1,) + (1,) * (len(shape) - 1 - dim))
    return factor_of


def normal_values(stream_key, extent, width, most, shards=(), kind=jnp.bfloat16):
    gain = block_levels(stream_key, extent, shards, -0.22, 0.18) if shards else 1.0
    result = jax.random.normal(stream_key, extent, jnp.float32) * width * gain
    return jnp.minimum(jnp.maximum(result, -most), most).astype(kind)


def setup_inputs(seed: int = 0) -> dict:
    keys = jax.random.split(jax.random.key(seed), 6)
    return {
        "ranges": jnp.clip(jnp.exp(math.log(1.0) - 4.61031033 * jax.random.uniform(keys[0], (BATCH, OUTW), jnp.float32) ** block_levels(keys[0], (BATCH, OUTW), ((0, 32),), -0.2, 0.2)), 0.0099487305, 1.0).astype(jnp.bfloat16),
        "board": draw_board(jax.random.fold_in(keys[5], 71), 0),
        "targets": normal_values(keys[2], (BATCH, OUTW), 1.0, 6.0, ((0, 32),)),
        "w_in": normal_values(keys[3], (HIDDEN_SIZE, INW), (3.0 * INW ** -0.5), 0.34570312, ((0, 32),)),
        "w_out": normal_values(keys[4], (HIDDEN_SIZE, OUTW), (2.0 * HIDDEN_SIZE ** -0.5), 0.3046875, ((0, 32),)),
    }


def huber_terms(error_value):
    magnitude = jnp.abs(error_value)
    return jnp.where(magnitude <= 1.0, 0.5 * error_value * error_value, magnitude - 0.5)

def reference(ranges, board, targets, w_in, w_out):
    card_ids = jnp.arange(CARDS, dtype=jnp.int32)
    onehot_board = lax.optimization_barrier(jnp.sum((board[:, :, None] == card_ids[None, None, :]).astype(jnp.float32), axis=1)).astype(jnp.bfloat16)
    features = jnp.concatenate([ranges, onehot_board], axis=1)
    preact = lax.dot_general(features, w_in, (((1,), (1,)), ((), ())), preferred_element_type=jnp.float32)
    hidden = jax.nn.gelu(preact).astype(jnp.bfloat16)
    group_width = HIDDEN_SIZE // N_MP
    summed = jnp.zeros((ranges.shape[0], w_out.shape[1]), jnp.float32)
    for group in range(N_MP):
        part_value = jnp.dot(hidden[:, group * group_width:(group + 1) * group_width], w_out[group * group_width:(group + 1) * group_width], preferred_element_type=jnp.float32)
        rounded = lax.optimization_barrier(part_value.astype(jnp.bfloat16))
        summed = summed + rounded.astype(jnp.float32)
    predicted = summed.astype(jnp.bfloat16)
    error_value = summed - targets.astype(jnp.float32)
    loss = jnp.sum(huber_terms(error_value)) / (ranges.shape[0] * w_out.shape[1])
    out_grad = jnp.clip(error_value, -1.0, 1.0).astype(jnp.bfloat16)
    grad_out = lax.dot_general(hidden, out_grad, (((0,), (0,)), ((), ())), preferred_element_type=jnp.float32)
    hidden_grad = lax.dot_general(out_grad, w_out, (((1,), (1,)), ((), ())), preferred_element_type=jnp.float32)
    unused_value, gelu_back = jax.vjp(jax.nn.gelu, preact)
    preact_grad = gelu_back(hidden_grad)[0].astype(jnp.bfloat16)
    grad_in = lax.dot_general(preact_grad, features, (((0,), (0,)), ((), ())), preferred_element_type=jnp.float32)
    square_sum = jnp.sum(grad_in * grad_in) + jnp.sum(grad_out * grad_out)
    count_params = HIDDEN_SIZE * (w_in.shape[1] + w_out.shape[1])
    scale = lax.rsqrt(square_sum / count_params + 1e-06)
    return (predicted, grad_in * scale, grad_out * scale, loss)
```

```python
import functools

import jax
import jax.numpy as jnp
from jax import lax
from jax.experimental import pallas as pl
from jax.experimental.pallas import tpu as pltpu
from jax.sharding import PartitionSpec as P

CARDS = 52
MESH = pl.DeviceIdType.MESH
GELU_K = 0.7978845608028654
GELU_C = 0.044715


def huber_terms(error_value):
    magnitude = jnp.abs(error_value)
    return jnp.where(magnitude <= 1.0, 0.5 * error_value * error_value, magnitude - 0.5)


def dot_nt(a, b):
    return lax.dot_general(a, b, (((1,), (1,)), ((), ())), preferred_element_type=jnp.float32)


def dot_nn(a, b):
    return lax.dot_general(a, b, (((1,), (0,)), ((), ())), preferred_element_type=jnp.float32)


def column_chunks(width, count):
    tiles = -(-width // 128)
    edges = [min(width, 128 * (-(-tiles * k // count))) for k in range(count + 1)]
    return [pl.ds(a, b - a) for a, b in zip(edges[:-1], edges[1:]) if b > a]


def step_kernel(
    dp, mp, chunks,
    feat_ref, targets_ref, w_in_ref, w_out_ref,
    pred_ref, gin_ref, gout_ref, stat_ref,
    feats, ogs, og_own, win, wout, preact, hidden, partial,
    sp, lp, sr, rr, sl, rl, sgo, lgo, sgi, lgi,
    w_sem, ag1, ag2, p_sem, r_sem, l_sem, g_sem,
):
    chips = dp // 2
    n_right, n_left = chips // 2, (chips - 1) // 2
    rows = feat_ref.shape[0]
    units = w_in_ref.shape[0]
    me = lax.axis_index("dp")
    me_mp = lax.axis_index("mp")
    core = me % 2
    chip = me // 2
    odd = chip % 2
    pos = (1 - odd) * (chip // 2) + odd * (chips - 1 - chip // 2)

    def dp_at(rel, core_index):
        there = (pos + rel + chips) % chips
        half = there // (chips // 2)
        where = (1 - half) * (2 * there) + half * (2 * (chips - 1 - there) + 1)
        return where * 2 + core_index

    right = (dp_at(1, core), me_mp)
    left = (dp_at(-1, core), me_mp)
    partner = (chip * 2 + 1 - core, me_mp)
    peers = [(me, (me_mp + j) % mp) for j in range(1, mp)]
    back_peers = [(me, (me_mp - j + mp) % mp) for j in range(1, mp)]

    barrier = pltpu.get_barrier_semaphore()
    greeted = [right, left, partner] + peers
    for other in greeted:
        pl.semaphore_signal(barrier, inc=1, device_id=other, device_id_type=MESH)
    pl.semaphore_wait(barrier, len(greeted))

    def block(rel, core_index):
        return pl.ds(pl.multiple_of(dp_at(rel, core_index) * rows, rows), rows)

    def send(src, dst, sems, index, device):
        copy = pltpu.make_async_remote_copy(
            src_ref=src, dst_ref=dst,
            send_sem=sems.at[(0,) + index], recv_sem=sems.at[(1,) + index],
            device_id=device, device_id_type=MESH,
        )
        copy.start()
        return copy

    def start_gather(own_ref, buf, sems):
        pieces = column_chunks(buf.shape[1], chunks)
        here = block(0, core)
        first = {}
        for k, piece in enumerate(pieces):
            first["r", k] = send(own_ref.at[:, piece], buf.at[here, piece], sems, (0, 0, k), right)
            first["l", k] = send(own_ref.at[:, piece], buf.at[here, piece], sems, (1, 0, k), left)
        first["p"] = [
            send(own_ref.at[:, piece], buf.at[here, piece], sems, (2, 0, k), partner)
            for k, piece in enumerate(pieces)
        ]
        return first

    def finish_gather(own_ref, buf, sems, first):
        pieces = column_chunks(buf.shape[1], chunks)
        here = block(0, core)
        buf[here, :] = own_ref[...]
        flying = {k: v for k, v in first.items() if k != "p"}
        done = []
        partner_copies = list(first["p"])
        count = 1
        for s in range(n_right):
            coming = {}
            for side, steps, sign, lane, device in (
                ("r", n_right, -1, 0, right), ("l", n_left, 1, 1, left)
            ):
                if s >= steps:
                    continue
                spot = block(sign * (s + 1), core)
                for k, piece in enumerate(pieces):
                    copy = flying[side, k]
                    copy.wait_recv()
                    done.append(copy)
                    part = buf.at[spot, piece]
                    if s + 1 < steps:
                        coming[side, k] = send(part, part, sems, (lane, s + 1, k), device)
                    partner_copies.append(send(part, part, sems, (2, count, k), partner))
                count += 1
            flying = coming
        for copy in partner_copies:
            copy.wait_recv()
        for copy in done + partner_copies:
            copy.wait_send()

    first = start_gather(feat_ref, feats, ag1)
    weight_copies = []
    for j, device in enumerate(back_peers):
        weight_copies.append(send(w_in_ref, win.at[j + 1], w_sem, (0, j), device))
        weight_copies.append(send(w_out_ref, wout.at[j + 1], w_sem, (1, j), device))
    win[0] = w_in_ref[...]
    wout[0] = w_out_ref[...]
    finish_gather(feat_ref, feats, ag1, first)
    for copy in weight_copies:
        copy.wait()

    all_units = mp * units
    win_all = win[...].reshape(all_units, win.shape[2])
    pre = dot_nt(feats[...], win_all)
    preact[...] = pre
    tanh_value = jnp.tanh(GELU_K * (pre + GELU_C * pre * pre * pre))
    hidden_value = 0.5 * pre * (1.0 + tanh_value)
    hidden[...] = hidden_value.astype(jnp.bfloat16)
    partial[...] = dot_nn(hidden[...], wout[...].reshape(all_units, wout.shape[2]))

    order = []
    for s in range(n_right):
        order.append(n_right - s)
        if s < n_left:
            order.append(-(n_left - s))
    order.append(0)
    shared = {}
    for k, rel in enumerate(order):
        sp[k] = partial[block(rel, 1 - core), :].astype(jnp.bfloat16)
        shared[rel] = (k, send(sp.at[k], lp.at[k], p_sem, (k,), partner))

    def contribution(rel):
        k, copy = shared[rel]
        copy.wait_recv()
        return partial[block(rel, core), :] + lp[k].astype(jnp.float32)

    right_copies, left_copies = [], []
    for s in range(n_right):
        total = contribution(n_right - s)
        if s:
            right_copies[-1].wait_recv()
            total = total + rr[s - 1].astype(jnp.float32)
        sr[s] = total.astype(jnp.bfloat16)
        right_copies.append(send(sr.at[s], rr.at[s], r_sem, (s,), right))
        if s < n_left:
            total = contribution(-(n_left - s))
            if s:
                left_copies[-1].wait_recv()
                total = total + rl[s - 1].astype(jnp.float32)
            sl[s] = total.astype(jnp.bfloat16)
            left_copies.append(send(sl.at[s], rl.at[s], l_sem, (s,), left))
    summed = contribution(0)
    right_copies[-1].wait_recv()
    summed = summed + rr[n_right - 1].astype(jnp.float32)
    left_copies[-1].wait_recv()
    summed = summed + rl[n_left - 1].astype(jnp.float32)

    error_value = summed - targets_ref[...].astype(jnp.float32)
    og_own[...] = jnp.clip(error_value, -1.0, 1.0).astype(jnp.bfloat16)
    first = start_gather(og_own, ogs, ag2)
    pred_ref[...] = summed.astype(jnp.bfloat16)
    loss_part = jnp.sum(huber_terms(error_value))
    pre = preact[...]
    tanh_value = jnp.tanh(GELU_K * (pre + GELU_C * pre * pre * pre))
    slope = 0.5 * (1.0 + tanh_value) + 0.5 * pre * (1.0 - tanh_value * tanh_value) * (
        GELU_K * (1.0 + 3.0 * GELU_C * pre * pre)
    )
    hidden_t = jnp.transpose(hidden[...].astype(jnp.float32)).astype(jnp.bfloat16)
    for _, copy in shared.values():
        copy.wait_send()
    for copy in right_copies + left_copies:
        copy.wait_send()
    finish_gather(og_own, ogs, ag2, first)

    grad_copies = []
    go = dot_nn(hidden_t, ogs[...])
    for j, device in enumerate(peers):
        sgo[j] = go[(j + 1) * units:(j + 2) * units, :].astype(jnp.bfloat16)
        grad_copies.append(send(sgo.at[j], lgo.at[j], g_sem, (0, j), device))
    gout_ref[...] = go[:units, :]
    hidden_grad = dot_nt(ogs[...], wout[...].reshape(all_units, wout.shape[2]))
    preact_grad = jnp.transpose(hidden_grad * slope).astype(jnp.bfloat16)
    gi = dot_nn(preact_grad, feats[...])
    for j, device in enumerate(peers):
        sgi[j] = gi[(j + 1) * units:(j + 2) * units, :].astype(jnp.bfloat16)
        grad_copies.append(send(sgi.at[j], lgi.at[j], g_sem, (1, j), device))
    gin_ref[...] = gi[:units, :]
    for copy in grad_copies:
        copy.wait()
    go_own = gout_ref[...]
    gi_own = gin_ref[...]
    for j in range(mp - 1):
        go_own = go_own + lgo[j].astype(jnp.float32)
        gi_own = gi_own + lgi[j].astype(jnp.float32)
    gout_ref[...] = go_own
    gin_ref[...] = gi_own
    squares = jnp.sum(gi_own * gi_own) + jnp.sum(go_own * go_own)
    row = lax.broadcasted_iota(jnp.int32, stat_ref.shape, 0)
    stat_ref[...] = jnp.where(row == 0, loss_part, squares)


def body(ranges, board, targets, w_in, w_out):
    mp = lax.axis_size("mp")
    dp = lax.axis_size("dp")
    rows, out_w = targets.shape
    units_real, in_w = w_in.shape
    pad = -units_real % 16
    if pad:
        w_in = jnp.pad(w_in, ((0, pad), (0, 0)))
        w_out = jnp.pad(w_out, ((0, pad), (0, 0)))
    units = units_real + pad
    card_ids = jnp.arange(CARDS, dtype=jnp.int32)
    onehot = jnp.any(board[:, :, None] == card_ids[None, None, :], axis=1).astype(jnp.bfloat16)
    features = jnp.concatenate([ranges, onehot], axis=1)

    chips = dp // 2
    n_right, n_left = chips // 2, (chips - 1) // 2
    chunks = 2
    batch = dp * rows
    all_units = mp * units
    bf16, f32 = jnp.bfloat16, jnp.float32
    vmem = pltpu.VMEM
    dma = pltpu.SemaphoreType.DMA
    pred, gin, gout, stat = pl.pallas_call(
        functools.partial(step_kernel, dp, mp, chunks),
        out_shape=[
            jax.ShapeDtypeStruct((rows, out_w), bf16),
            jax.ShapeDtypeStruct((units, in_w), f32),
            jax.ShapeDtypeStruct((units, out_w), f32),
            jax.ShapeDtypeStruct((8, 128), f32),
        ],
        in_specs=[pl.BlockSpec(memory_space=vmem)] * 4,
        out_specs=[pl.BlockSpec(memory_space=vmem)] * 4,
        scratch_shapes=[
            vmem((batch, in_w), bf16),
            vmem((batch, out_w), bf16),
            vmem((rows, out_w), bf16),
            vmem((mp, units, in_w), bf16),
            vmem((mp, units, out_w), bf16),
            vmem((batch, all_units), f32),
            vmem((batch, all_units), bf16),
            vmem((batch, out_w), f32),
            vmem((chips, rows, out_w), bf16),
            vmem((chips, rows, out_w), bf16),
            vmem((n_right, rows, out_w), bf16),
            vmem((n_right, rows, out_w), bf16),
            vmem((n_left, rows, out_w), bf16),
            vmem((n_left, rows, out_w), bf16),
            vmem((mp - 1, units, out_w), bf16),
            vmem((mp - 1, units, out_w), bf16),
            vmem((mp - 1, units, in_w), bf16),
            vmem((mp - 1, units, in_w), bf16),
            dma((2, 2, mp - 1)),
            dma((2, 3, chips, chunks)),
            dma((2, 3, chips, chunks)),
            dma((2, chips)),
            dma((2, n_right)),
            dma((2, n_left)),
            dma((2, 2, mp - 1)),
        ],
        compiler_params=pltpu.CompilerParams(collective_id=0, has_side_effects=True),
        name="step",
    )(features, targets, w_in, w_out)
    stats = lax.all_gather(stat[:2, :1], ("dp", "mp"), axis=1, tiled=True)
    totals = jnp.sum(stats, axis=1)
    count_params = units_real * mp * dp * (in_w + out_w)
    scale = lax.rsqrt(totals[1] / count_params + 1e-06)
    loss = totals[0] / (rows * mp * dp * out_w)
    return (pred, gin[:units_real] * scale, gout[:units_real] * scale, loss)


def solution(mesh):
    in_specs = (
        P(("dp", "mp"), None),
        P(("dp", "mp"), None),
        P(("dp", "mp"), None),
        P(("mp", "dp"), None),
        P(("mp", "dp"), None),
    )
    out_specs = (P(("dp", "mp"), None), P(("mp", "dp"), None), P(("mp", "dp"), None), P())
    return jax.shard_map(body, mesh=mesh, in_specs=in_specs, out_specs=out_specs, check_vma=False)
```

```python
import functools

import jax
import jax.numpy as jnp
from jax import lax
from jax.experimental import pallas as pl
from jax.experimental.pallas import tpu as pltpu
from jax.sharding import PartitionSpec as P

CARDS = 52
MESH = pl.DeviceIdType.MESH
GELU_K = 0.7978845608028654
GELU_C = 0.044715


def huber_terms(error_value):
    magnitude = jnp.abs(error_value)
    return jnp.where(magnitude <= 1.0, 0.5 * error_value * error_value, magnitude - 0.5)


def dot_nt(a, b):
    return lax.dot_general(a, b, (((1,), (1,)), ((), ())), preferred_element_type=jnp.float32)


def dot_nn(a, b):
    return lax.dot_general(a, b, (((1,), (0,)), ((), ())), preferred_element_type=jnp.float32)


def column_chunks(width, count):
    tiles = -(-width // 128)
    edges = [min(width, 128 * (-(-tiles * k // count))) for k in range(count + 1)]
    return [pl.ds(a, b - a) for a, b in zip(edges[:-1], edges[1:]) if b > a]


def dot_tn(a, b):
    return lax.dot_general(a, b, (((0,), (0,)), ((), ())), preferred_element_type=jnp.float32)


def step_kernel(
    dp, mp, chunks, count_params, count_values,
    ranges_ref, board_ref, targets_ref, w_in_ref, w_out_ref,
    pred_ref, gin_ref, gout_ref, stat_ref,
    feat_own, feats, ogs, og_own, win, wout, preact, hidden, partial, go_acc, gi_acc,
    sp, lp, sr, rr, sl, rl, sgo, lgo, sgi, lgi, st, ld1, st2, ld2,
    w_sem, ag1, ag2, p_sem, r_sem, l_sem, g_sem, s1_sem, s2_sem,
):
    chips = dp // 2
    steps = chips // 2
    rows = ranges_ref.shape[0]
    units = w_in_ref.shape[0]
    me = lax.axis_index("dp")
    me_mp = lax.axis_index("mp")
    core = me % 2
    chip = me // 2
    odd = chip % 2
    pos = (1 - odd) * (chip // 2) + odd * (chips - 1 - chip // 2)

    def at(rel):
        there = (pos + rel + chips) % chips
        half = there // (chips // 2)
        where = (1 - half) * (2 * there) + half * (2 * (chips - 1 - there) + 1)
        return (where * 2 + core, me_mp)

    right, left = at(1), at(-1)
    partner = (chip * 2 + 1 - core, me_mp)
    peers = [(me, (me_mp + j) % mp) for j in range(1, mp)]
    back_peers = [(me, (me_mp - j + mp) % mp) for j in range(1, mp)]
    line = [at(r) for r in range(1, chips)]
    square = [
        (chip * 2 + (core + c) % 2, (me_mp + j) % mp)
        for c in range(2) for j in range(mp) if c or j
    ]

    barrier = pltpu.get_barrier_semaphore()
    for other in line + square:
        pl.semaphore_signal(barrier, inc=1, device_id=other, device_id_type=MESH)

    cards = lax.broadcasted_iota(jnp.int32, (rows, CARDS), 1)
    onehot = jnp.zeros((rows, CARDS), jnp.float32)
    for k in range(board_ref.shape[1]):
        onehot = onehot + (board_ref[:, k:k + 1] == cards).astype(jnp.float32)
    feat_own[...] = jnp.concatenate(
        [ranges_ref[...].astype(jnp.float32), onehot], axis=1
    ).astype(jnp.bfloat16)
    pl.semaphore_wait(barrier, len(line + square))

    def send(src, dst, sems, index, device):
        copy = pltpu.make_async_remote_copy(
            src_ref=src, dst_ref=dst,
            send_sem=sems.at[(0,) + index], recv_sem=sems.at[(1,) + index],
            device_id=device, device_id_type=MESH,
        )
        copy.start()
        return copy

    def spot(slot, side):
        return pl.ds((2 * slot + side) * rows, rows)

    def half_of(side, count):
        return range(count // 2) if side == 0 else range(count // 2, count)

    def start_gather(own_ref, buf, sems):
        pieces = column_chunks(buf.shape[1], chunks)
        flying = {}
        last = steps == 1
        for k, piece in enumerate(pieces):
            for side, device in ((0, right), (1, left)):
                if last and k not in half_of(side, len(pieces)):
                    continue
                slot = 1 if last else 1 + side
                flying[side, k] = send(
                    own_ref.at[:, piece], buf.at[spot(slot, 0), piece], sems, (side, 0, k), device
                )
        own = [
            send(own_ref.at[:, piece], buf.at[spot(0, 1), piece], sems, (2, 0, k), partner)
            for k, piece in enumerate(pieces)
        ]
        return flying, own

    def finish_gather(own_ref, buf, sems, started, before_last):
        pieces = column_chunks(buf.shape[1], chunks)
        flying, partner_copies = started
        buf[spot(0, 0), :] = own_ref[...]
        done = []
        by_slot = {0: list(partner_copies)}
        for s in range(steps):
            coming = {}
            final, next_final = s == steps - 1, s == steps - 2
            for k, piece in enumerate(pieces):
                for side, device in ((0, right), (1, left)):
                    if (side, k) not in flying:
                        continue
                    copy = flying[side, k]
                    copy.wait_recv()
                    done.append(copy)
                    slot = 2 * s + 1 if final else 2 * s + 1 + side
                    part = buf.at[spot(slot, 0), piece]
                    if not final and not (next_final and k not in half_of(side, len(pieces))):
                        target = 2 * s + 3 if next_final else 2 * s + 3 + side
                        coming[side, k] = send(
                            part, buf.at[spot(target, 0), piece], sems, (side, s + 1, k), device
                        )
                    by_slot.setdefault(slot, []).append(
                        send(part, buf.at[spot(slot, 1), piece], sems, (2, slot, k), partner)
                    )
            flying = coming
            if next_final:
                for slot in range(chips - 1):
                    for copy in by_slot[slot]:
                        copy.wait_recv()
                before_last()
        for copy in by_slot[chips - 1]:
            copy.wait_recv()
        for copy in done + [c for cs in by_slot.values() for c in cs]:
            copy.wait_send()

    started = start_gather(feat_own, feats, ag1)
    in_copies = [
        send(w_in_ref, win.at[j + 1], w_sem, (0, j), device) for j, device in enumerate(back_peers)
    ]
    out_copies = [
        send(w_out_ref, wout.at[j + 1], w_sem, (1, j), device) for j, device in enumerate(back_peers)
    ]
    win[0] = w_in_ref[...]
    wout[0] = w_out_ref[...]
    all_units = mp * units
    batch = dp * rows
    split = 2 * rows * (chips - 1)
    middle = batch // 2

    def hidden_rows(a, b):
        pre = dot_nt(feats[a:b, :], win[...].reshape(all_units, win.shape[2]))
        preact[a:b, :] = pre
        tanh_value = jnp.tanh(GELU_K * (pre + GELU_C * pre * pre * pre))
        hidden[a:b, :] = (0.5 * pre * (1.0 + tanh_value)).astype(jnp.bfloat16)

    def early_hidden():
        for copy in in_copies:
            copy.wait()
        hidden_rows(0, split)

    finish_gather(feat_own, feats, ag1, started, early_hidden)
    hidden_rows(split, batch)
    for copy in out_copies:
        copy.wait()
    shared = {}
    for a, b in ((middle, batch), (0, middle)):
        partial[a:b, :] = dot_nn(hidden[a:b, :], wout[...].reshape(all_units, wout.shape[2]))
        for slot in reversed(range(a // (2 * rows), b // (2 * rows))):
            sp[slot] = partial[spot(slot, 1), :].astype(jnp.bfloat16)
            shared[slot] = send(sp.at[slot], lp.at[slot], p_sem, (slot,), partner)

    pieces = column_chunks(partial.shape[1], chunks)

    def contribution(slot, piece):
        return partial[spot(slot, 0), piece] + lp[slot, :, piece].astype(jnp.float32)

    sums = {}
    sides = ((0, sr, rr, r_sem, right), (1, sl, rl, l_sem, left))
    waited = set()
    for s in range(steps):
        for k, piece in enumerate(pieces):
            for side, outgoing, landed, sems, device in sides:
                if s == 0 and k not in half_of(side, len(pieces)):
                    continue
                distance = steps - s
                slot = chips - 1 if s == 0 else (2 * distance if side == 0 else 2 * distance - 1)
                if slot not in waited:
                    shared[slot].wait_recv()
                    waited.add(slot)
                total = contribution(slot, piece)
                if (side, s - 1, k) in sums:
                    sums[side, s - 1, k].wait_recv()
                    total = total + landed[s - 1, :, piece].astype(jnp.float32)
                outgoing[s, :, piece] = total.astype(jnp.bfloat16)
                sums[side, s, k] = send(
                    outgoing.at[s, :, piece], landed.at[s, :, piece], sems, (s, k), device
                )
    shared[0].wait_recv()
    loss_part = 0.0
    for k, piece in enumerate(pieces):
        total = contribution(0, piece)
        for side, outgoing, landed, sems, device in sides:
            if (side, steps - 1, k) in sums:
                sums[side, steps - 1, k].wait_recv()
                total = total + landed[steps - 1, :, piece].astype(jnp.float32)
        pred_ref[:, piece] = total.astype(jnp.bfloat16)
        error_value = total - targets_ref[:, piece].astype(jnp.float32)
        og_own[:, piece] = jnp.clip(error_value, -1.0, 1.0).astype(jnp.bfloat16)
        loss_part = loss_part + jnp.sum(huber_terms(error_value))
    started = start_gather(og_own, ogs, ag2)
    pre = preact[...]
    tanh_value = jnp.tanh(GELU_K * (pre + GELU_C * pre * pre * pre))
    preact[...] = 0.5 * (1.0 + tanh_value) + 0.5 * pre * (1.0 - tanh_value * tanh_value) * (
        GELU_K * (1.0 + 3.0 * GELU_C * pre * pre)
    )
    for copy in list(shared.values()) + list(sums.values()):
        copy.wait_send()

    def early_grads():
        back = dot_nt(ogs[:split, :], wout[...].reshape(all_units, wout.shape[2]))
        pre_grad = (back * preact[:split, :]).astype(jnp.bfloat16)
        go_acc[...] = dot_tn(hidden[:split, :], ogs[:split, :])
        gi_acc[...] = dot_tn(pre_grad, feats[:split, :])

    finish_gather(og_own, ogs, ag2, started, early_grads)

    grad_copies = []

    def ship(acc, late, staged, landed, lane, out_ref):
        for j, device in enumerate(peers):
            mine = slice((j + 1) * units, (j + 2) * units)
            staged[j] = (acc[mine, :] + late[mine, :]).astype(jnp.bfloat16)
            grad_copies.append(send(staged.at[j], landed.at[j], g_sem, (lane, j), device))
        out_ref[...] = acc[:units, :] + late[:units, :]

    ship(go_acc, dot_tn(hidden[split:, :], ogs[split:, :]), sgo, lgo, 0, gout_ref)
    back = dot_nt(ogs[split:, :], wout[...].reshape(all_units, wout.shape[2]))
    pre_grad = (back * preact[split:, :]).astype(jnp.bfloat16)
    ship(gi_acc, dot_tn(pre_grad, feats[split:, :]), sgi, lgi, 1, gin_ref)

    def own_total(out_ref, landed, lane):
        for copy in grad_copies[lane * (mp - 1):(lane + 1) * (mp - 1)]:
            copy.wait()
        total = out_ref[...]
        for j in range(mp - 1):
            total = total + landed[j].astype(jnp.float32)
        out_ref[...] = total
        return jnp.sum(total * total)

    squares = own_total(gout_ref, lgo, 0)
    squares = squares + own_total(gin_ref, lgi, 1)
    row = lax.broadcasted_iota(jnp.int32, stat_ref.shape, 0)
    st[...] = jnp.where(row == 0, loss_part, squares)
    copies = [
        send(st, ld1.at[r], s1_sem, (r,), device) for r, device in enumerate(line)
    ]
    total = st[...]
    for r, copy in enumerate(copies):
        copy.wait()
        total = total + ld1[r]
    st2[...] = total
    copies = [
        send(st2, ld2.at[r], s2_sem, (r,), device) for r, device in enumerate(square)
    ]
    for r, copy in enumerate(copies):
        copy.wait()
        total = total + ld2[r]
    stat_ref[...] = jnp.where(
        row == 0, total / count_values, lax.rsqrt(total / count_params + 1e-06)
    )


def body(ranges, board, targets, w_in, w_out):
    mp = lax.axis_size("mp")
    dp = lax.axis_size("dp")
    rows, out_w = targets.shape
    units_real, in_w = w_in.shape
    pad = -units_real % 16
    if pad:
        w_in = jnp.pad(w_in, ((0, pad), (0, 0)))
        w_out = jnp.pad(w_out, ((0, pad), (0, 0)))
    units = units_real + pad
    chips = dp // 2
    steps = chips // 2
    chunks = 4
    batch = dp * rows
    all_units = mp * units
    bf16, f32 = jnp.bfloat16, jnp.float32
    vmem = pltpu.VMEM
    dma = pltpu.SemaphoreType.DMA
    count_params = units_real * mp * dp * (in_w + out_w)
    count_values = rows * mp * dp * out_w
    pred, gin, gout, stat = pl.pallas_call(
        functools.partial(step_kernel, dp, mp, chunks, count_params, count_values),
        out_shape=[
            jax.ShapeDtypeStruct((rows, out_w), bf16),
            jax.ShapeDtypeStruct((units, in_w), f32),
            jax.ShapeDtypeStruct((units, out_w), f32),
            jax.ShapeDtypeStruct((8, 128), f32),
        ],
        in_specs=[pl.BlockSpec(memory_space=vmem)] * 5,
        out_specs=[pl.BlockSpec(memory_space=vmem)] * 4,
        scratch_shapes=[
            vmem((rows, in_w), bf16),
            vmem((batch, in_w), bf16),
            vmem((batch, out_w), bf16),
            vmem((rows, out_w), bf16),
            vmem((mp, units, in_w), bf16),
            vmem((mp, units, out_w), bf16),
            vmem((batch, all_units), f32),
            vmem((batch, all_units), bf16),
            vmem((batch, out_w), f32),
            vmem((all_units, out_w), f32),
            vmem((all_units, in_w), f32),
            vmem((chips, rows, out_w), bf16),
            vmem((chips, rows, out_w), bf16),
            vmem((steps, rows, out_w), bf16),
            vmem((steps, rows, out_w), bf16),
            vmem((steps, rows, out_w), bf16),
            vmem((steps, rows, out_w), bf16),
            vmem((mp - 1, units, out_w), bf16),
            vmem((mp - 1, units, out_w), bf16),
            vmem((mp - 1, units, in_w), bf16),
            vmem((mp - 1, units, in_w), bf16),
            vmem((8, 128), f32),
            vmem((chips - 1, 8, 128), f32),
            vmem((8, 128), f32),
            vmem((2 * mp - 1, 8, 128), f32),
            dma((2, 2, mp - 1)),
            dma((2, 3, chips, chunks)),
            dma((2, 3, chips, chunks)),
            dma((2, chips)),
            dma((2, steps, chunks)),
            dma((2, steps, chunks)),
            dma((2, 2, mp - 1)),
            dma((2, chips - 1)),
            dma((2, 2 * mp - 1)),
        ],
        compiler_params=pltpu.CompilerParams(collective_id=0, has_side_effects=True),
        name="step",
    )(ranges, board, targets, w_in, w_out)
    scale = stat[1:2, :1]
    return (pred, gin[:units_real] * scale, gout[:units_real] * scale, stat[0, 0])


def solution(mesh):
    in_specs = (
        P(("dp", "mp"), None),
        P(("dp", "mp"), None),
        P(("dp", "mp"), None),
        P(("mp", "dp"), None),
        P(("mp", "dp"), None),
    )
    out_specs = (P(("dp", "mp"), None), P(("mp", "dp"), None), P(("mp", "dp"), None), P())
    return jax.shard_map(body, mesh=mesh, in_specs=in_specs, out_specs=out_specs, check_vma=False)
```

```python
import functools

import jax
import jax.numpy as jnp
from jax import lax
from jax.experimental import pallas as pl
from jax.experimental.pallas import tpu as pltpu
from jax.sharding import PartitionSpec as P

CARDS = 52
MESH = pl.DeviceIdType.MESH
GELU_K = 0.7978845608028654
GELU_C = 0.044715


def huber_terms(error_value):
    magnitude = jnp.abs(error_value)
    return jnp.where(magnitude <= 1.0, 0.5 * error_value * error_value, magnitude - 0.5)


def dot_nt(a, b):
    return lax.dot_general(a, b, (((1,), (1,)), ((), ())), preferred_element_type=jnp.float32)


def dot_nn(a, b):
    return lax.dot_general(a, b, (((1,), (0,)), ((), ())), preferred_element_type=jnp.float32)


def column_chunks(width, count):
    tiles = -(-width // 128)
    edges = [min(width, 128 * (-(-tiles * k // count))) for k in range(count + 1)]
    return [pl.ds(a, b - a) for a, b in zip(edges[:-1], edges[1:]) if b > a]


def dot_tn(a, b):
    return lax.dot_general(a, b, (((0,), (0,)), ((), ())), preferred_element_type=jnp.float32)


def step_kernel(
    dp, mp, chunks, swap, count_params, count_values,
    ranges_ref, board_ref, targets_ref, w_in_ref, w_out_ref,
    pred_ref, gin_ref, gout_ref, stat_ref,
    feat_own, feats, ogs, og_own, win, wout, preact, hidden, partial, go_acc, gi_acc,
    sp, lp, sr, rr, sl, rl, sgo, lgo, sgi, lgi, st, ld1, st2, ld2, pf, spg, lpg,
    w_sem, ag1, ag2, p_sem, r_sem, l_sem, g_sem, s1_sem, s2_sem, f_sem, pg_sem,
):
    chips = dp // 2
    steps = chips // 2
    rows = ranges_ref.shape[0]
    units = w_in_ref.shape[0]
    me = lax.axis_index("dp")
    me_mp = lax.axis_index("mp")
    core = me % 2
    chip = me // 2
    odd = chip % 2
    pos = (1 - odd) * (chip // 2) + odd * (chips - 1 - chip // 2)

    def at(rel):
        there = (pos + rel + chips) % chips
        half = there // (chips // 2)
        where = (1 - half) * (2 * there) + half * (2 * (chips - 1 - there) + 1)
        return (where * 2 + core, me_mp)

    right, left = at(1), at(-1)
    partner = (chip * 2 + 1 - core, me_mp)
    peers = [(me, (me_mp + j) % mp) for j in range(1, mp)]
    back_peers = [(me, (me_mp - j + mp) % mp) for j in range(1, mp)]
    line = [at(r) for r in range(1, chips)]
    square = [
        (chip * 2 + (core + c) % 2, (me_mp + j) % mp)
        for c in range(2) for j in range(mp) if c or j
    ]

    barrier = pltpu.get_barrier_semaphore()
    for other in line + square:
        pl.semaphore_signal(barrier, inc=1, device_id=other, device_id_type=MESH)

    cards = lax.broadcasted_iota(jnp.int32, (CARDS, rows), 0)
    onehot = jnp.zeros((CARDS, rows), jnp.float32)
    for k in range(board_ref.shape[0]):
        onehot = onehot + (board_ref[k:k + 1, :] == cards).astype(jnp.float32)
    feat_own[...] = jnp.concatenate(
        [ranges_ref[...].astype(jnp.float32), jnp.transpose(onehot)], axis=1
    ).astype(jnp.bfloat16)
    pl.semaphore_wait(barrier, len(line + square))

    def send(src, dst, sems, index, device):
        copy = pltpu.make_async_remote_copy(
            src_ref=src, dst_ref=dst,
            send_sem=sems.at[(0,) + index], recv_sem=sems.at[(1,) + index],
            device_id=device, device_id_type=MESH,
        )
        copy.start()
        return copy

    def spot(slot, side):
        return pl.ds((2 * slot + side) * rows, rows)

    def half_of(side, count):
        return range(count // 2) if side == 0 else range(count // 2, count)

    def start_gather(own_ref, buf, sems):
        pieces = column_chunks(buf.shape[1], chunks)
        flying = {}
        last = steps == 1
        for k, piece in enumerate(pieces):
            for side, device in ((0, right), (1, left)):
                if last and k not in half_of(side, len(pieces)):
                    continue
                slot = 1 if last else 1 + side
                flying[side, k] = send(
                    own_ref.at[:, piece], buf.at[spot(slot, 0), piece], sems, (side, 0, k), device
                )
        own = [
            send(own_ref.at[:, piece], buf.at[spot(0, 1), piece], sems, (2, 0, k), partner)
            for k, piece in enumerate(pieces)
        ]
        return flying, own

    def finish_gather(own_ref, buf, sems, started, before_last):
        pieces = column_chunks(buf.shape[1], chunks)
        flying, partner_copies = started
        buf[spot(0, 0), :] = own_ref[...]
        done = []
        by_slot = {0: list(partner_copies)}
        for s in range(steps):
            coming = {}
            final, next_final = s == steps - 1, s == steps - 2
            for k, piece in enumerate(pieces):
                for side, device in ((0, right), (1, left)):
                    if (side, k) not in flying:
                        continue
                    copy = flying[side, k]
                    copy.wait_recv()
                    done.append(copy)
                    slot = 2 * s + 1 if final else 2 * s + 1 + side
                    part = buf.at[spot(slot, 0), piece]
                    if not final and not (next_final and k not in half_of(side, len(pieces))):
                        target = 2 * s + 3 if next_final else 2 * s + 3 + side
                        coming[side, k] = send(
                            part, buf.at[spot(target, 0), piece], sems, (side, s + 1, k), device
                        )
                    by_slot.setdefault(slot, []).append(
                        send(part, buf.at[spot(slot, 1), piece], sems, (2, slot, k), partner)
                    )
            flying = coming
            if next_final:
                for slot in range(chips - 1):
                    for copy in by_slot[slot]:
                        copy.wait_recv()
                before_last()
        for copy in by_slot[chips - 1]:
            copy.wait_recv()
        for copy in done + [c for cs in by_slot.values() for c in cs]:
            copy.wait_send()

    started = start_gather(feat_own, feats, ag1)
    in_copies = [
        send(w_in_ref, win.at[j + 1], w_sem, (0, j), device) for j, device in enumerate(back_peers)
    ]
    out_copies = [
        send(w_out_ref, wout.at[j + 1], w_sem, (1, j), device) for j, device in enumerate(back_peers)
    ]
    win[0] = w_in_ref[...]
    wout[0] = w_out_ref[...]
    all_units = mp * units
    batch = dp * rows
    split = 2 * rows * (chips - 1)
    middle = batch // 2

    def hidden_rows(a, b):
        pre = dot_nt(feats[a:b, :], win[...].reshape(all_units, win.shape[2]))
        preact[a:b, :] = pre
        tanh_value = jnp.tanh(GELU_K * (pre + GELU_C * pre * pre * pre))
        hidden[a:b, :] = (0.5 * pre * (1.0 + tanh_value)).astype(jnp.bfloat16)

    def early_hidden():
        for copy in in_copies:
            copy.wait()
        hidden_rows(0, split)

    finish_gather(feat_own, feats, ag1, started, early_hidden)
    feat_copies = []
    if swap:
        feat_copies = [
            send(feats, pf.at[j], f_sem, (j,), device) for j, device in enumerate(peers)
        ]
    hidden_rows(split, batch)
    for copy in out_copies:
        copy.wait()
    shared = {}
    for a, b in ((middle, batch), (0, middle)):
        partial[a:b, :] = dot_nn(hidden[a:b, :], wout[...].reshape(all_units, wout.shape[2]))
        for slot in reversed(range(a // (2 * rows), b // (2 * rows))):
            sp[slot] = partial[spot(slot, 1), :].astype(jnp.bfloat16)
            shared[slot] = send(sp.at[slot], lp.at[slot], p_sem, (slot,), partner)

    pieces = column_chunks(partial.shape[1], chunks)

    def contribution(slot, piece):
        return partial[spot(slot, 0), piece] + lp[slot, :, piece].astype(jnp.float32)

    sums = {}
    sides = ((0, sr, rr, r_sem, right), (1, sl, rl, l_sem, left))
    waited = set()
    for s in range(steps):
        for k, piece in enumerate(pieces):
            for side, outgoing, landed, sems, device in sides:
                if s == 0 and k not in half_of(side, len(pieces)):
                    continue
                distance = steps - s
                slot = chips - 1 if s == 0 else (2 * distance if side == 0 else 2 * distance - 1)
                if slot not in waited:
                    shared[slot].wait_recv()
                    waited.add(slot)
                total = contribution(slot, piece)
                if (side, s - 1, k) in sums:
                    sums[side, s - 1, k].wait_recv()
                    total = total + landed[s - 1, :, piece].astype(jnp.float32)
                outgoing[s, :, piece] = total.astype(jnp.bfloat16)
                sums[side, s, k] = send(
                    outgoing.at[s, :, piece], landed.at[s, :, piece], sems, (s, k), device
                )
    shared[0].wait_recv()
    loss_part = 0.0
    for k, piece in enumerate(pieces):
        total = contribution(0, piece)
        for side, outgoing, landed, sems, device in sides:
            if (side, steps - 1, k) in sums:
                sums[side, steps - 1, k].wait_recv()
                total = total + landed[steps - 1, :, piece].astype(jnp.float32)
        pred_ref[:, piece] = total.astype(jnp.bfloat16)
        error_value = total - targets_ref[:, piece].astype(jnp.float32)
        og_own[:, piece] = jnp.clip(error_value, -1.0, 1.0).astype(jnp.bfloat16)
        loss_part = loss_part + jnp.sum(huber_terms(error_value))
    started = start_gather(og_own, ogs, ag2)
    pre = preact[...]
    tanh_value = jnp.tanh(GELU_K * (pre + GELU_C * pre * pre * pre))
    preact[...] = 0.5 * (1.0 + tanh_value) + 0.5 * pre * (1.0 - tanh_value * tanh_value) * (
        GELU_K * (1.0 + 3.0 * GELU_C * pre * pre)
    )
    for copy in list(shared.values()) + list(sums.values()):
        copy.wait_send()

    pg_copies = []

    def swap_pre_grad(pre_grad, lane, a, b):
        for j, device in enumerate(peers):
            spg[j, a:b, :] = pre_grad[:, (j + 1) * units:(j + 2) * units]
            pg_copies.append(send(
                spg.at[j, pl.ds(a, b - a)], lpg.at[j, pl.ds(a, b - a)], pg_sem, (lane, j), device
            ))

    def early_grads():
        back = dot_nt(ogs[:split, :], wout[...].reshape(all_units, wout.shape[2]))
        pre_grad = (back * preact[:split, :]).astype(jnp.bfloat16)
        go_acc[...] = dot_tn(hidden[:split, :], ogs[:split, :])
        if swap:
            gin_ref[...] = dot_tn(pre_grad[:, :units], feats[:split, :])
            swap_pre_grad(pre_grad, 0, 0, split)
        else:
            gi_acc[...] = dot_tn(pre_grad, feats[:split, :])

    finish_gather(og_own, ogs, ag2, started, early_grads)

    grad_copies = []

    def ship(acc, late, staged, landed, lane, out_ref):
        for j, device in enumerate(peers):
            mine = slice((j + 1) * units, (j + 2) * units)
            staged[j] = (acc[mine, :] + late[mine, :]).astype(jnp.bfloat16)
            grad_copies.append(send(staged.at[j], landed.at[j], g_sem, (lane, j), device))
        out_ref[...] = acc[:units, :] + late[:units, :]

    if not swap:
        ship(go_acc, dot_tn(hidden[split:, :], ogs[split:, :]), sgo, lgo, 0, gout_ref)
    back = dot_nt(ogs[split:, :], wout[...].reshape(all_units, wout.shape[2]))
    pre_grad = (back * preact[split:, :]).astype(jnp.bfloat16)
    if swap:
        swap_pre_grad(pre_grad, 1, split, batch)
        ship(go_acc, dot_tn(hidden[split:, :], ogs[split:, :]), sgo, lgo, 0, gout_ref)
        gin_ref[...] = gin_ref[...] + dot_tn(pre_grad[:, :units], feats[split:, :])
        for copy in feat_copies + pg_copies:
            copy.wait()
        for j in range(mp - 1):
            gin_ref[...] = gin_ref[...] + dot_tn(lpg[j], pf[j])
        squares = jnp.sum(gin_ref[...] * gin_ref[...])
    else:
        ship(gi_acc, dot_tn(pre_grad, feats[split:, :]), sgi, lgi, 1, gin_ref)

    def own_total(out_ref, landed, lane):
        for copy in grad_copies[lane * (mp - 1):(lane + 1) * (mp - 1)]:
            copy.wait()
        total = out_ref[...]
        for j in range(mp - 1):
            total = total + landed[j].astype(jnp.float32)
        out_ref[...] = total
        return jnp.sum(total * total)

    if not swap:
        squares = own_total(gin_ref, lgi, 1)
    squares = squares + own_total(gout_ref, lgo, 0)
    row = lax.broadcasted_iota(jnp.int32, st.shape, 0)
    st[...] = jnp.where(row == 0, loss_part, squares)
    copies = [
        send(st, ld1.at[r], s1_sem, (r,), device) for r, device in enumerate(line)
    ]
    total = st[...]
    for r, copy in enumerate(copies):
        copy.wait()
        total = total + ld1[r]
    st2[...] = total
    copies = [
        send(st2, ld2.at[r], s2_sem, (r,), device) for r, device in enumerate(square)
    ]
    for r, copy in enumerate(copies):
        copy.wait()
        total = total + ld2[r]
    stat_ref[...] = total[0:1, 0:1] / count_values
    scale = lax.rsqrt(total[1:2, 0:1] / count_params + 1e-06)
    gout_ref[...] = gout_ref[...] * scale
    gin_ref[...] = gin_ref[...] * scale


def body(ranges, board, targets, w_in, w_out):
    mp = lax.axis_size("mp")
    dp = lax.axis_size("dp")
    rows, out_w = targets.shape
    units_real, in_w = w_in.shape
    pad = -units_real % 16
    if pad:
        w_in = jnp.pad(w_in, ((0, pad), (0, 0)))
        w_out = jnp.pad(w_out, ((0, pad), (0, 0)))
    units = units_real + pad
    chips = dp // 2
    steps = chips // 2
    chunks = 4
    swap = (mp - 1) * dp * rows * in_w * 2 <= 8 * 2**20
    batch = dp * rows
    all_units = mp * units
    bf16, f32 = jnp.bfloat16, jnp.float32
    vmem = pltpu.VMEM
    dma = pltpu.SemaphoreType.DMA
    count_params = units_real * mp * dp * (in_w + out_w)
    count_values = rows * mp * dp * out_w
    pred, gin, gout, stat = pl.pallas_call(
        functools.partial(step_kernel, dp, mp, chunks, swap, count_params, count_values),
        out_shape=[
            jax.ShapeDtypeStruct((rows, out_w), bf16),
            jax.ShapeDtypeStruct((units, in_w), f32),
            jax.ShapeDtypeStruct((units, out_w), f32),
            jax.ShapeDtypeStruct((1, 1), f32),
        ],
        in_specs=[pl.BlockSpec(memory_space=vmem)] * 5,
        out_specs=[pl.BlockSpec(memory_space=vmem)] * 4,
        scratch_shapes=[
            vmem((rows, in_w), bf16),
            vmem((batch, in_w), bf16),
            vmem((batch, out_w), bf16),
            vmem((rows, out_w), bf16),
            vmem((mp, units, in_w), bf16),
            vmem((mp, units, out_w), bf16),
            vmem((batch, all_units), f32),
            vmem((batch, all_units), bf16),
            vmem((batch, out_w), f32),
            vmem((all_units, out_w), f32),
            vmem((all_units, in_w), f32),
            vmem((chips, rows, out_w), bf16),
            vmem((chips, rows, out_w), bf16),
            vmem((steps, rows, out_w), bf16),
            vmem((steps, rows, out_w), bf16),
            vmem((steps, rows, out_w), bf16),
            vmem((steps, rows, out_w), bf16),
            vmem((mp - 1, units, out_w), bf16),
            vmem((mp - 1, units, out_w), bf16),
            vmem((mp - 1, units, in_w), bf16),
            vmem((mp - 1, units, in_w), bf16),
            vmem((8, 128), f32),
            vmem((chips - 1, 8, 128), f32),
            vmem((8, 128), f32),
            vmem((2 * mp - 1, 8, 128), f32),
            vmem((mp - 1, batch, in_w) if swap else (1, 8, 128), bf16),
            vmem((mp - 1, batch, units) if swap else (1, 8, 128), bf16),
            vmem((mp - 1, batch, units) if swap else (1, 8, 128), bf16),
            dma((2, 2, mp - 1)),
            dma((2, 3, chips, chunks)),
            dma((2, 3, chips, chunks)),
            dma((2, chips)),
            dma((2, steps, chunks)),
            dma((2, steps, chunks)),
            dma((2, 2, mp - 1)),
            dma((2, chips - 1)),
            dma((2, 2 * mp - 1)),
            dma((2, mp - 1)),
            dma((2, 2, mp - 1)),
        ],
        compiler_params=pltpu.CompilerParams(collective_id=0, has_side_effects=True),
        name="step",
    )(ranges, board.T, targets, w_in, w_out)
    if pad:
        gin, gout = gin[:units_real], gout[:units_real]
    return (pred, gin, gout, stat.reshape(()))


def solution(mesh):
    in_specs = (
        P(("dp", "mp"), None),
        P(("dp", "mp"), None),
        P(("dp", "mp"), None),
        P(("mp", "dp"), None),
        P(("mp", "dp"), None),
    )
    out_specs = (P(("dp", "mp"), None), P(("mp", "dp"), None), P(("mp", "dp"), None), P())
    return jax.shard_map(body, mesh=mesh, in_specs=in_specs, out_specs=out_specs, check_vma=False)
```

```python
import functools

import jax
import jax.numpy as jnp
from jax import lax
from jax.experimental import pallas as pl
from jax.experimental.pallas import tpu as pltpu
from jax.sharding import PartitionSpec as P

CARDS = 52
MESH = pl.DeviceIdType.MESH
GELU_K = 0.7978845608028654
GELU_C = 0.044715


def huber_terms(error_value):
    magnitude = jnp.abs(error_value)
    return jnp.where(magnitude <= 1.0, 0.5 * error_value * error_value, magnitude - 0.5)


def dot_nt(a, b):
    return lax.dot_general(a, b, (((1,), (1,)), ((), ())), preferred_element_type=jnp.float32)


def dot_nn(a, b):
    return lax.dot_general(a, b, (((1,), (0,)), ((), ())), preferred_element_type=jnp.float32)


def column_chunks(width, count):
    tiles = -(-width // 128)
    edges = [min(width, 128 * (-(-tiles * k // count))) for k in range(count + 1)]
    return [pl.ds(a, b - a) for a, b in zip(edges[:-1], edges[1:]) if b > a]


def dot_tn(a, b):
    return lax.dot_general(a, b, (((0,), (0,)), ((), ())), preferred_element_type=jnp.float32)


def step_kernel(
    dp, mp, chunks, swap, count_params, count_values,
    ranges_ref, board_ref, targets_ref, w_in_ref, w_out_ref,
    pred_ref, gin_ref, gout_ref, stat_ref,
    feat_own, feats, ogs, og_own, win, wout, preact, hidden, partial, go_acc, gi_acc,
    sp, lp, sr, rr, sl, rl, sgo, lgo, sgi, lgi, st, ld1, st2, ld2, pf, spg, lpg,
    w_sem, ag1, ag2, p_sem, r_sem, l_sem, g_sem, s1_sem, s2_sem, f_sem, pg_sem,
):
    chips = dp // 2
    steps = chips // 2
    rows = ranges_ref.shape[0]
    units = w_in_ref.shape[0]
    me = lax.axis_index("dp")
    me_mp = lax.axis_index("mp")
    core = me % 2
    chip = me // 2
    odd = chip % 2
    pos = (1 - odd) * (chip // 2) + odd * (chips - 1 - chip // 2)

    def at(rel):
        there = (pos + rel + chips) % chips
        half = there // (chips // 2)
        where = (1 - half) * (2 * there) + half * (2 * (chips - 1 - there) + 1)
        return (where * 2 + core, me_mp)

    right, left = at(1), at(-1)
    partner = (chip * 2 + 1 - core, me_mp)
    peers = [(me, (me_mp + j) % mp) for j in range(1, mp)]
    back_peers = [(me, (me_mp - j + mp) % mp) for j in range(1, mp)]
    line = [at(r) for r in range(1, chips)]
    square = [
        (chip * 2 + (core + c) % 2, (me_mp + j) % mp)
        for c in range(2) for j in range(mp) if c or j
    ]

    barrier = pltpu.get_barrier_semaphore()
    for other in line + square:
        pl.semaphore_signal(barrier, inc=1, device_id=other, device_id_type=MESH)

    cards = lax.broadcasted_iota(jnp.int32, (CARDS, rows), 0)
    onehot = jnp.zeros((CARDS, rows), jnp.float32)
    for k in range(board_ref.shape[0]):
        onehot = onehot + (board_ref[k:k + 1, :] == cards).astype(jnp.float32)
    feat_own[...] = jnp.concatenate(
        [ranges_ref[...].astype(jnp.float32), jnp.transpose(onehot)], axis=1
    ).astype(jnp.bfloat16)
    pl.semaphore_wait(barrier, len(line + square))

    def send(src, dst, sems, index, device):
        copy = pltpu.make_async_remote_copy(
            src_ref=src, dst_ref=dst,
            send_sem=sems.at[(0,) + index], recv_sem=sems.at[(1,) + index],
            device_id=device, device_id_type=MESH,
        )
        copy.start()
        return copy

    def spot(slot, side):
        return pl.ds((2 * slot + side) * rows, rows)

    def half_of(side, count):
        return range(count // 2) if side == 0 else range(count // 2, count)

    def start_gather(own_ref, buf, sems):
        pieces = column_chunks(buf.shape[1], chunks)
        flying = {}
        last = steps == 1
        for k, piece in enumerate(pieces):
            for side, device in ((0, right), (1, left)):
                if last and k not in half_of(side, len(pieces)):
                    continue
                slot = 1 if last else 1 + side
                flying[side, k] = send(
                    own_ref.at[:, piece], buf.at[spot(slot, 0), piece], sems, (side, 0, k), device
                )
        own = [
            send(own_ref.at[:, piece], buf.at[spot(0, 1), piece], sems, (2, 0, k), partner)
            for k, piece in enumerate(pieces)
        ]
        return flying, own

    def finish_gather(own_ref, buf, sems, started, before_last):
        pieces = column_chunks(buf.shape[1], chunks)
        flying, partner_copies = started
        buf[spot(0, 0), :] = own_ref[...]
        done = []
        by_slot = {0: list(partner_copies)}
        for s in range(steps):
            coming = {}
            final, next_final = s == steps - 1, s == steps - 2
            for k, piece in enumerate(pieces):
                for side, device in ((0, right), (1, left)):
                    if (side, k) not in flying:
                        continue
                    copy = flying[side, k]
                    copy.wait_recv()
                    done.append(copy)
                    slot = 2 * s + 1 if final else 2 * s + 1 + side
                    part = buf.at[spot(slot, 0), piece]
                    if not final and not (next_final and k not in half_of(side, len(pieces))):
                        target = 2 * s + 3 if next_final else 2 * s + 3 + side
                        coming[side, k] = send(
                            part, buf.at[spot(target, 0), piece], sems, (side, s + 1, k), device
                        )
                    by_slot.setdefault(slot, []).append(
                        send(part, buf.at[spot(slot, 1), piece], sems, (2, slot, k), partner)
                    )
            flying = coming
            if next_final:
                for slot in range(chips - 1):
                    for copy in by_slot[slot]:
                        copy.wait_recv()
                before_last()
        for copy in by_slot[chips - 1]:
            copy.wait_recv()
        for copy in done + [c for cs in by_slot.values() for c in cs]:
            copy.wait_send()

    started = start_gather(feat_own, feats, ag1)
    in_copies = [
        send(w_in_ref, win.at[j + 1], w_sem, (0, j), device) for j, device in enumerate(back_peers)
    ]
    out_copies = [
        send(w_out_ref, wout.at[j + 1], w_sem, (1, j), device) for j, device in enumerate(back_peers)
    ]
    win[0] = w_in_ref[...]
    wout[0] = w_out_ref[...]
    all_units = mp * units
    batch = dp * rows
    split = 2 * rows * (chips - 1)
    middle = batch // 2

    def hidden_rows(a, b):
        pre = dot_nt(feats[a:b, :], win[...].reshape(all_units, win.shape[2]))
        preact[a:b, :] = pre
        tanh_value = jnp.tanh(GELU_K * (pre + GELU_C * pre * pre * pre))
        hidden[a:b, :] = (0.5 * pre * (1.0 + tanh_value)).astype(jnp.bfloat16)

    def early_hidden():
        for copy in in_copies:
            copy.wait()
        hidden_rows(0, split)

    finish_gather(feat_own, feats, ag1, started, early_hidden)
    feat_copies = []
    if swap:
        feat_copies = [
            send(feats, pf.at[j], f_sem, (j,), device) for j, device in enumerate(peers)
        ]
    hidden_rows(split, batch)
    for copy in out_copies:
        copy.wait()
    shared = {}
    for a, b in ((middle, batch), (0, middle)):
        partial[a:b, :] = dot_nn(hidden[a:b, :], wout[...].reshape(all_units, wout.shape[2]))
        for slot in reversed(range(a // (2 * rows), b // (2 * rows))):
            sp[slot] = partial[spot(slot, 1), :].astype(jnp.bfloat16)
            shared[slot] = send(sp.at[slot], lp.at[slot], p_sem, (slot,), partner)

    pieces = column_chunks(partial.shape[1], chunks)

    def contribution(slot, piece):
        return partial[spot(slot, 0), piece] + lp[slot, :, piece].astype(jnp.float32)

    sums = {}
    sides = ((0, sr, rr, r_sem, right), (1, sl, rl, l_sem, left))
    waited = set()
    for s in range(steps):
        for k, piece in enumerate(pieces):
            for side, outgoing, landed, sems, device in sides:
                if s == 0 and k not in half_of(side, len(pieces)):
                    continue
                distance = steps - s
                slot = chips - 1 if s == 0 else (2 * distance if side == 0 else 2 * distance - 1)
                if slot not in waited:
                    shared[slot].wait_recv()
                    waited.add(slot)
                total = contribution(slot, piece)
                if (side, s - 1, k) in sums:
                    sums[side, s - 1, k].wait_recv()
                    total = total + landed[s - 1, :, piece].astype(jnp.float32)
                outgoing[s, :, piece] = total.astype(jnp.bfloat16)
                sums[side, s, k] = send(
                    outgoing.at[s, :, piece], landed.at[s, :, piece], sems, (s, k), device
                )
    shared[0].wait_recv()
    loss_part = 0.0
    for k, piece in enumerate(pieces):
        total = contribution(0, piece)
        for side, outgoing, landed, sems, device in sides:
            if (side, steps - 1, k) in sums:
                sums[side, steps - 1, k].wait_recv()
                total = total + landed[steps - 1, :, piece].astype(jnp.float32)
        pred_ref[:, piece] = total.astype(jnp.bfloat16)
        error_value = total - targets_ref[:, piece].astype(jnp.float32)
        og_own[:, piece] = jnp.clip(error_value, -1.0, 1.0).astype(jnp.bfloat16)
        loss_part = loss_part + jnp.sum(huber_terms(error_value))
    started = start_gather(og_own, ogs, ag2)
    pre = preact[...]
    tanh_value = jnp.tanh(GELU_K * (pre + GELU_C * pre * pre * pre))
    preact[...] = 0.5 * (1.0 + tanh_value) + 0.5 * pre * (1.0 - tanh_value * tanh_value) * (
        GELU_K * (1.0 + 3.0 * GELU_C * pre * pre)
    )
    for copy in list(shared.values()) + list(sums.values()):
        copy.wait_send()

    pg_copies = []

    def swap_pre_grad(pre_grad, lane, a, b):
        for j, device in enumerate(peers):
            spg[j, a:b, :] = pre_grad[:, (j + 1) * units:(j + 2) * units]
            pg_copies.append(send(
                spg.at[j, pl.ds(a, b - a)], lpg.at[j, pl.ds(a, b - a)], pg_sem, (lane, j), device
            ))

    def early_grads():
        back = dot_nt(ogs[:split, :], wout[...].reshape(all_units, wout.shape[2]))
        pre_grad = (back * preact[:split, :]).astype(jnp.bfloat16)
        go_acc[...] = dot_tn(hidden[:split, :], ogs[:split, :])
        if swap:
            gin_ref[...] = dot_tn(pre_grad[:, :units], feats[:split, :])
            swap_pre_grad(pre_grad, 0, 0, split)
        else:
            gi_acc[...] = dot_tn(pre_grad, feats[:split, :])

    finish_gather(og_own, ogs, ag2, started, early_grads)

    grad_copies = []

    def ship(acc, late, staged, landed, lane, out_ref):
        for j, device in enumerate(peers):
            mine = slice((j + 1) * units, (j + 2) * units)
            staged[j] = (acc[mine, :] + late[mine, :]).astype(jnp.bfloat16)
            grad_copies.append(send(staged.at[j], landed.at[j], g_sem, (lane, j), device))
        out_ref[...] = acc[:units, :] + late[:units, :]

    if not swap:
        ship(go_acc, dot_tn(hidden[split:, :], ogs[split:, :]), sgo, lgo, 0, gout_ref)
    back = dot_nt(ogs[split:, :], wout[...].reshape(all_units, wout.shape[2]))
    pre_grad = (back * preact[split:, :]).astype(jnp.bfloat16)
    if swap:
        swap_pre_grad(pre_grad, 1, split, batch)
        ship(go_acc, dot_tn(hidden[split:, :], ogs[split:, :]), sgo, lgo, 0, gout_ref)
        gin_ref[...] = gin_ref[...] + dot_tn(pre_grad[:, :units], feats[split:, :])
        for copy in feat_copies + pg_copies:
            copy.wait()
        for j in range(mp - 1):
            gin_ref[...] = gin_ref[...] + dot_tn(lpg[j], pf[j])
        squares = jnp.sum(gin_ref[...] * gin_ref[...])
    else:
        ship(gi_acc, dot_tn(pre_grad, feats[split:, :]), sgi, lgi, 1, gin_ref)

    def own_total(out_ref, landed, lane):
        for copy in grad_copies[lane * (mp - 1):(lane + 1) * (mp - 1)]:
            copy.wait()
        total = out_ref[...]
        for j in range(mp - 1):
            total = total + landed[j].astype(jnp.float32)
        out_ref[...] = total
        return jnp.sum(total * total)

    if not swap:
        squares = own_total(gin_ref, lgi, 1)
    squares = squares + own_total(gout_ref, lgo, 0)
    row = lax.broadcasted_iota(jnp.int32, st.shape, 0)
    st[...] = jnp.where(row == 0, loss_part, squares)
    copies = [
        send(st, ld1.at[r], s1_sem, (r,), device) for r, device in enumerate(line)
    ]
    total = st[...]
    for r, copy in enumerate(copies):
        copy.wait()
        total = total + ld1[r]
    st2[...] = total
    copies = [
        send(st2, ld2.at[r], s2_sem, (r,), device) for r, device in enumerate(square)
    ]
    for r, copy in enumerate(copies):
        copy.wait()
        total = total + ld2[r]
    stat_ref[...] = total[0:1, 0:1] / count_values
    scale = lax.rsqrt(total[1:2, 0:1] / count_params + 1e-06)
    gout_ref[...] = gout_ref[...] * scale
    gin_ref[...] = gin_ref[...] * scale


def body(ranges, board, targets, w_in, w_out):
    mp = lax.axis_size("mp")
    dp = lax.axis_size("dp")
    rows, out_w = targets.shape
    units_real, in_w = w_in.shape
    pad = -units_real % 16
    if pad:
        w_in = jnp.pad(w_in, ((0, pad), (0, 0)))
        w_out = jnp.pad(w_out, ((0, pad), (0, 0)))
    units = units_real + pad
    chips = dp // 2
    steps = chips // 2
    chunks = 2
    swap = (mp - 1) * dp * rows * in_w * 2 <= 8 * 2**20
    batch = dp * rows
    all_units = mp * units
    bf16, f32 = jnp.bfloat16, jnp.float32
    vmem = pltpu.VMEM
    dma = pltpu.SemaphoreType.DMA
    count_params = units_real * mp * dp * (in_w + out_w)
    count_values = rows * mp * dp * out_w
    pred, gin, gout, stat = pl.pallas_call(
        functools.partial(step_kernel, dp, mp, chunks, swap, count_params, count_values),
        out_shape=[
            jax.ShapeDtypeStruct((rows, out_w), bf16),
            jax.ShapeDtypeStruct((units, in_w), f32),
            jax.ShapeDtypeStruct((units, out_w), f32),
            jax.ShapeDtypeStruct((1, 1), f32),
        ],
        in_specs=[pl.BlockSpec(memory_space=vmem)] * 5,
        out_specs=[pl.BlockSpec(memory_space=vmem)] * 4,
        scratch_shapes=[
            vmem((rows, in_w), bf16),
            vmem((batch, in_w), bf16),
            vmem((batch, out_w), bf16),
            vmem((rows, out_w), bf16),
            vmem((mp, units, in_w), bf16),
            vmem((mp, units, out_w), bf16),
            vmem((batch, all_units), f32),
            vmem((batch, all_units), bf16),
            vmem((batch, out_w), f32),
            vmem((all_units, out_w), f32),
            vmem((all_units, in_w), f32),
            vmem((chips, rows, out_w), bf16),
            vmem((chips, rows, out_w), bf16),
            vmem((steps, rows, out_w), bf16),
            vmem((steps, rows, out_w), bf16),
            vmem((steps, rows, out_w), bf16),
            vmem((steps, rows, out_w), bf16),
            vmem((mp - 1, units, out_w), bf16),
            vmem((mp - 1, units, out_w), bf16),
            vmem((mp - 1, units, in_w), bf16),
            vmem((mp - 1, units, in_w), bf16),
            vmem((8, 128), f32),
            vmem((chips - 1, 8, 128), f32),
            vmem((8, 128), f32),
            vmem((2 * mp - 1, 8, 128), f32),
            vmem((mp - 1, batch, in_w) if swap else (1, 8, 128), bf16),
            vmem((mp - 1, batch, units) if swap else (1, 8, 128), bf16),
            vmem((mp - 1, batch, units) if swap else (1, 8, 128), bf16),
            dma((2, 2, mp - 1)),
            dma((2, 3, chips, chunks)),
            dma((2, 3, chips, chunks)),
            dma((2, chips)),
            dma((2, steps, chunks)),
            dma((2, steps, chunks)),
            dma((2, 2, mp - 1)),
            dma((2, chips - 1)),
            dma((2, 2 * mp - 1)),
            dma((2, mp - 1)),
            dma((2, 2, mp - 1)),
        ],
        compiler_params=pltpu.CompilerParams(collective_id=0, has_side_effects=True),
        name="step",
    )(ranges, board.T, targets, w_in, w_out)
    if pad:
        gin, gout = gin[:units_real], gout[:units_real]
    return (pred, gin, gout, stat.reshape(()))


def solution(mesh):
    in_specs = (
        P(("dp", "mp"), None),
        P(("dp", "mp"), None),
        P(("dp", "mp"), None),
        P(("mp", "dp"), None),
        P(("mp", "dp"), None),
    )
    out_specs = (P(("dp", "mp"), None), P(("mp", "dp"), None), P(("mp", "dp"), None), P())
    return jax.shard_map(body, mesh=mesh, in_specs=in_specs, out_specs=out_specs, check_vma=False)
```
